32 devices in a mesh: ends: 2 (over x), dp: 4 (over y, core), tp: 4 (over z).
Axes of the slice: x: 2, y: 2, z: 4, core: 2. Of those that a mesh axis runs over, the one named last changes fastest.
Arguments:
- grad: bfloat16 [2, 4, 4096, 3072], P('ends', 'dp', 'tp'), may hold values from -1800 to 1800
- master: float32 [4, 1024, 3072], P('tp', ('ends', 'dp')), may hold values from -3 to 3
- moment: float32 [4, 1024, 3072], P('tp', ('ends', 'dp')), may hold values from -3 to 3
- second: float32 [4, 1024, 3072], P('tp', ('ends', 'dp')), may hold values from 0.01 to 1
Outputs:
- weights: bfloat16 [4096, 3072], P('tp')
- master_out: float32 [4, 1024, 3072], P('tp', ('ends', 'dp'))
- moment_out: float32 [4, 1024, 3072], P('tp', ('ends', 'dp'))
- second_out: float32 [4, 1024, 3072], P('tp', ('ends', 'dp'))
The draws below stay inside these ranges and needn't reach their ends.
All inputs are finite; a program needn't handle non-finite values.
Results may differ from the reference program's by a relative error of at most 0.0034.
Values may be sent and summed in bfloat16 or wider, within the bound.
A program may use at most 128 MiB of HBM per device.

```python
import math
import jax
import jax.numpy as jnp
from jax import lax

D = 3072
STEP = 10
ROWS_TP = 1024
VOCAB = 4096
N_ENDS = 2
N_DP = 4
N_TP = 4


def draw_grad(key, part):
    keys = jax.random.split(jax.random.fold_in(key, 17), 4)
    shape = (N_ENDS, N_DP, VOCAB, D)
    base = jax.random.truncated_normal(keys[0], -4.0, 4.0, shape, jnp.float32)
    members = N_ENDS * N_DP
    member = 0.5 * 3.0 ** (jnp.arange(members, dtype=jnp.float32) / max(members - 1, 1))
    member = member.reshape(N_ENDS, N_DP, 1, 1)
    position = (jnp.arange(VOCAB, dtype=jnp.int32) % ROWS_TP).astype(jnp.float32) / ROWS_TP
    rough = jnp.exp(jax.random.uniform(keys[2], (VOCAB,), jnp.float32, 0.0, math.log(10.0)))
    row_scale = 3.0 ** position * rough
    col_scale = jnp.exp(jax.random.uniform(keys[3], (D,), jnp.float32, 0.0, math.log(10.0)))
    values = base * member * row_scale[None, None, :, None] * col_scale[None, None, None, :]
    return values.astype(jnp.bfloat16)


def block_scale(stream_key, extent, shards, low, largest):
    gain, own = 1.0, jax.random.fold_in(stream_key, 6)
    for axis_at, parts in shards:
        draws = jnp.exp(jax.random.uniform(jax.random.fold_in(own, axis_at), (parts,), jnp.float32, low / len(shards), largest / len(shards)))
        gain = gain * jnp.repeat(draws, extent[axis_at] // parts).reshape([-1 if axis == axis_at else 1 for axis in range(len(extent))])
    return gain


def scatter_about(key, extent, deviation, most, pieces=(), held_as=jnp.bfloat16):
    result = jax.random.normal(key, extent, jnp.float32) * deviation
    if len(pieces) > 0:
        result = block_scale(key, extent, pieces, -0.22, 0.18) * result
    return jnp.clip(result, min=-most, max=most).astype(held_as)


def setup_inputs(seed: int = 0) -> dict:
    streams_of = jax.random.split(jax.random.key(seed), 5)
    return {
        "grad": draw_grad(jax.random.fold_in(streams_of[4], 71), 0),
        "master": scatter_about(streams_of[1], (N_TP, ROWS_TP, D), 0.5, 3.0, ((0, 4), (1, 8)), jnp.float32),
        "moment": scatter_about(streams_of[2], (N_TP, ROWS_TP, D), 0.5, 3.0, ((0, 4), (1, 8)), jnp.float32),
        "second": jnp.clip(jnp.exp(math.log(1.0) - 4.6051702 * jax.random.uniform(streams_of[3], (N_TP, ROWS_TP, D), jnp.float32) ** block_scale(streams_of[3], (N_TP, ROWS_TP, D), ((0, 4), (1, 8)), -0.2, 0.2)), 0.01, 1.0),
    }


def reference(grad, master, moment, second):
    stacked = grad.reshape(N_ENDS * N_DP, VOCAB, D)

    def accumulate(carry, member):
        return (carry + member.astype(jnp.float32), None)
    summed, _ = lax.scan(accumulate, jnp.zeros((VOCAB, D), jnp.float32), stacked)
    norm = jnp.sqrt(jnp.sum(summed * summed))
    factor = jnp.minimum(jnp.float32(1.0), jnp.sqrt(jnp.float32(VOCAB * D)) / (norm + 1e-06))
    clipped = (factor * summed).reshape(N_TP, ROWS_TP, D)
    moment_out = 0.9 * moment + 0.1 * clipped
    second_out = 0.999 * second + 0.001 * clipped * clipped
    update = moment_out / (1.0 - 0.9 ** STEP) / (jnp.sqrt(second_out / (1.0 - 0.999 ** STEP)) + 1e-08)
    master_out = master - 0.01 * (update + 0.1 * master)
    weights = master_out.reshape(VOCAB, D).astype(jnp.bfloat16)
    return (weights, master_out, moment_out, second_out)
```

```python
import functools
import math

import jax
import jax.numpy as jnp
from jax import lax
from jax.experimental import pallas as pl
from jax.experimental.pallas import tpu as pltpu
from jax.sharding import PartitionSpec as P

STEP = 10
MESH = pl.DeviceIdType.MESH
F32 = jnp.float32
BF16 = jnp.bfloat16


def remote(src, dst, send, recv, device):
    return pltpu.make_async_remote_copy(
        src_ref=src, dst_ref=dst, send_sem=send, recv_sem=recv, device_id=device, device_id_type=MESH
    )


def kernel(cfg, grad, master, moment, second, w_out, master_out, moment_out, second_out, *scratch):
    ends, ys, tps, rows, width, cuts, staged = cfg
    if staged:
        w_hbm, (w_out, w_sem), scratch = w_out, scratch[-2:], scratch[:-2]
    (own, peer, part1, land1, part2, land2, total, st0, st1, st2, squares,
     own_sem, st_sem, peer_s, peer_r, s1, r1, s2, r2, ns, nr, a_s, a_r, b_s, b_r, f_s, f_r, p_s, p_r,
     up, down, here_p, here_1, here_2) = scratch
    e, dp, t = lax.axis_index("ends"), lax.axis_index("dp"), lax.axis_index("tp")
    y, c = dp // 2, lax.rem(dp, 2)
    pieces = len(cuts)
    devices = ends * ys * 2 * tps
    square = ends == ys
    n1, n2 = (ends, ys) if square else (ys, ends)

    def place(core, da, db):
        if square:
            ends_first = core == 0
            de, dy = jnp.where(ends_first, da, db), jnp.where(ends_first, db, da)
        else:
            de, dy = db, da
        return lax.rem(e + de, ends), lax.rem(y + dy, ys)

    def first_row(core, da, db):
        ee, yy = place(core, da, db)
        return pl.multiple_of(((ee * ys + yy) * 2 + core) * rows, rows)

    def at(da, db):
        ee, yy = place(c, da, db)
        return {"ends": ee, "dp": yy * 2 + c}

    partner = {"dp": y * 2 + (1 - c)}
    shifts1, shifts2 = range(1, n1), range(1, n2)
    order = (
        [(da, db) for da in shifts1 for db in shifts2]
        + [(0, db) for db in shifts2]
        + [(da, 0) for da in shifts1]
        + [(0, 0)]
    )
    slot = lambda da, db: da * n2 + db
    part = lambda k: pl.ds(*cuts[k])

    me = (e * (ys * 2) + dp) * tps + t
    barrier = pltpu.get_barrier_semaphore()
    signal = lambda sem, device: pl.semaphore_signal(sem, inc=1, device_id=device, device_id_type=MESH)
    planes = [at(da, 0) for da in shifts1], [at(0, db) for db in shifts2]
    above, below = {"tp": t + 1}, {"tp": t - 1}
    has_above, has_below = t < tps - 1, t > 0

    for device in planes[0] + planes[1] + [partner]:
        signal(barrier, device)
    pl.when(has_above)(lambda: signal(barrier, above))
    pl.when(has_below)(lambda: signal(barrier, below))

    def rows_at(start, k):
        first, size = cuts[k]
        return pl.ds(pl.multiple_of(start + first, 16), size)

    def own_copy(da, db, k):
        i = slot(da, db)
        return pltpu.make_async_copy(grad.at[rows_at(first_row(c, da, db), k)], own.at[i, part(k)], own_sem.at[i * pieces + k])

    for da, db in order:
        for k in range(pieces):
            own_copy(da, db, k).start()
    state_copies = [
        pltpu.make_async_copy(src, dst, st_sem.at[i])
        for i, (src, dst) in enumerate(((master, st0), (moment, st1), (second, st2)))
    ]
    pl.semaphore_wait(barrier, n1 + n2 - 1 + has_above.astype(jnp.int32) + has_below.astype(jnp.int32))

    for da, db in order:
        for k in range(pieces):
            i = slot(da, db)
            remote(grad.at[rows_at(first_row(1 - c, da, db), k)], peer.at[i, part(k)], peer_s, peer_r.at[i * pieces + k], partner).start()
    for copy in state_copies:
        copy.start()
    pl.when(jnp.logical_and(has_above, t == 0))(lambda: signal(up, above))
    pl.when(jnp.logical_and(has_below, t == tps - 1))(lambda: signal(down, below))

    def meet(step):
        if step == 0:
            @pl.when(has_below)
            def _():
                pl.semaphore_wait(up, 1)
                pl.when(has_above)(lambda: signal(up, above))
        if step == 1:
            @pl.when(has_above)
            def _():
                pl.semaphore_wait(down, 1)
                pl.when(has_below)(lambda: signal(down, below))
            signal(here_p, partner)
        if step == 2:
            pl.semaphore_wait(here_p, 1)
            for device in planes[0]:
                signal(here_1, device)
        if step == 3:
            pl.semaphore_wait(here_1, n1 - 1)
            for device in planes[1]:
                signal(here_2, device)
        if step == 4:
            pl.semaphore_wait(here_2, n2 - 1)

    def chip_sum(da, db, k):
        i = slot(da, db)
        own_copy(da, db, k).wait()
        remote(peer.at[i, part(k)], peer.at[i, part(k)], peer_s, peer_r.at[i * pieces + k], partner).wait_recv()
        return own[i, part(k), :].astype(F32) + peer[i, part(k), :].astype(F32)

    def copy1(da, db, k):
        i = (da - 1) * n2 + db
        return remote(part1.at[i, part(k)], land1.at[i, part(k)], s1, r1.at[i * pieces + k], at(da, 0))

    def copy2(db, k):
        i = db - 1
        return remote(part2.at[i, part(k)], land2.at[i, part(k)], s2, r2.at[i * pieces + k], at(0, db))

    def send1(da, db, k):
        part1[(da - 1) * n2 + db, part(k), :] = chip_sum(da, db, k).astype(BF16)
        copy1(da, db, k).start()

    def sum1(db, k):
        value = chip_sum(0, db, k)
        for da in shifts1:
            copy1(da, db, k).wait_recv()
            value = value + land1[(da - 1) * n2 + db, part(k), :].astype(F32)
        return value

    for k in range(pieces):
        for da in shifts1:
            for db in shifts2:
                send1(da, db, k)
    for k in range(pieces):
        for da in shifts1:
            send1(da, 0, k)
        for db in shifts2:
            part2[db - 1, part(k), :] = sum1(db, k).astype(BF16)
            copy2(db, k).start()
        if k < 3:
            meet(k)
    for step in range(min(pieces, 3), 4):
        meet(step)
    meet(4)
    acc = jnp.zeros((8, width), F32)
    for k in range(pieces):
        value = sum1(0, k)
        for db in shifts2:
            copy2(db, k).wait_recv()
            value = value + land2[db - 1, part(k), :].astype(F32)
        total[part(k), :] = value
        value = value * value
        for r in range(0, cuts[k][1], 8):
            acc = acc + value[r : r + 8, :]

    mine = acc[:, :128]
    for j in range(128, width, 128):
        mine = mine + acc[:, j : j + 128]
    squares[me] = jnp.sum(mine, axis=0, keepdims=True)

    high = t >= tps // 2
    for j in range(tps - 1):
        up_from, down_from = j + (t <= j).astype(jnp.int32), tps - 1 - j - (t >= tps - 1 - j).astype(jnp.int32)
        for de in range(ends):
            for ddp in range(ys * 2):
                device = {"ends": lax.rem(e + de, ends), "dp": lax.rem(dp + ddp, ys * 2), "tp": jnp.where(high, up_from, down_from)}
                remote(squares.at[me], squares.at[me], ns, nr, device).start()
    for de in range(ends):
        for ddp in range(ys * 2):
            if de or ddp:
                device = {"ends": lax.rem(e + de, ends), "dp": lax.rem(dp + ddp, ys * 2)}
                remote(squares.at[me], squares.at[me], ns, nr, device).start()

    others = squares.at[pl.ds(0, devices - 1)]
    everyone = remote(others, others, ns, nr, partner)
    for copy in state_copies:
        copy.wait()
    everyone.wait_recv()
    everyone.wait_send()
    norm2 = jnp.full((8, 128), jnp.sum(jnp.sum(squares[...], axis=0)), F32)
    entries = float(tps * ends * ys * 2 * rows * width)
    factor = jnp.minimum(F32(1.0), F32(math.sqrt(entries)) / (jnp.sqrt(norm2) + 1e-06))[:1, :1]

    my_row = first_row(c, 0, 0)

    def piece_of(da, db, k):
        return w_out.at[rows_at(first_row(c, da, db), k)]

    def copy_a(da, src, k):
        return remote(src, src, a_s, a_r.at[(da - 1) * pieces + k], at(da, 0))

    def copy_b(db, src, k):
        return remote(src, src, b_s, b_r.at[(db - 1) * pieces + k], at(0, db))

    def copy_f(da, db, src, k):
        return remote(src, src, f_s, f_r.at[((da - 1) * (n2 - 1) + db - 1) * pieces + k], at(0, db))

    def copy_p(src):
        return remote(src, src, p_s, p_r, partner)

    for k in range(pieces):
        @pl.loop(0, cuts[k][1] // 16)
        def _(g):
            at_row = pl.multiple_of(cuts[k][0] + g * 16, 16)
            here = pl.ds(at_row, 16)
            clipped = factor * total[here, :]
            m = 0.9 * st1[here, :] + 0.1 * clipped
            v = 0.999 * st2[here, :] + 0.001 * clipped * clipped
            update = m / (1.0 - 0.9**STEP) / (jnp.sqrt(v / (1.0 - 0.999**STEP)) + 1e-08)
            w = st0[here, :]
            w = w - 0.01 * (update + 0.1 * w)
            moment_out[here, :] = m
            second_out[here, :] = v
            master_out[here, :] = w
            w_out[pl.ds(pl.multiple_of(my_row + at_row, 16), 16), :] = w.astype(BF16)

        src = piece_of(0, 0, k)
        for da in shifts1:
            copy_a(da, src, k).start()
        for db in shifts2:
            copy_b(db, src, k).start()
        copy_p(src).start()

    for k in range(pieces):
        for da in shifts1:
            src = piece_of(n1 - da, 0, k)
            copy_a(da, src, k).wait_recv()
            for db in shifts2:
                copy_f(da, db, src, k).start()
            copy_p(src).start()
        for db in shifts2:
            src = piece_of(0, n2 - db, k)
            copy_b(db, src, k).wait_recv()
            copy_p(src).start()
    for k in range(pieces):
        for da in shifts1:
            for db in shifts2:
                src = piece_of(n1 - da, n2 - db, k)
                copy_f(da, db, src, k).wait_recv()
                copy_p(src).start()

    half = w_out.at[pl.ds(0, n1 * n2 * rows)]
    remote(half, half, p_s, p_r, partner).wait_recv()
    remote(half, half, p_s, p_r, partner).wait_send()
    remote(peer, peer, peer_s, peer_r.at[0], partner).wait_send()
    remote(part1, land1, s1, r1.at[0], partner).wait_send()
    remote(part2, land2, s2, r2.at[0], partner).wait_send()
    for sem, count, recv in ((a_s, n1 - 1, a_r), (b_s, n2 - 1, b_r), (f_s, (n1 - 1) * (n2 - 1), f_r)):
        ref = w_out.at[pl.ds(0, count * rows)]
        remote(ref, ref, sem, recv.at[0], partner).wait_send()
    if staged:
        final = pltpu.make_async_copy(w_out, w_hbm, w_sem)
        final.start()
        final.wait()


def put_out(*refs):
    count = len(refs) // 2
    sems = refs[-1]
    copies = [
        pltpu.make_async_copy(src, dst, sems.at[i])
        for i, (src, dst) in enumerate(zip(refs[:count], refs[count : 2 * count]))
    ]
    for copy in copies:
        copy.start()
    for copy in copies:
        copy.wait()


def per_device(mesh, grad, master, moment, second):
    ends, dps, tps = (mesh.shape[name] for name in ("ends", "dp", "tp"))
    ys = dps // 2
    rows_tp, width = grad.shape[2:]
    rows = rows_tp // (ends * dps)
    sizes = [16] + [32] * (rows // 32 - 1) + [16] if rows % 32 == 0 and rows >= 64 else [rows]
    cuts = tuple((sum(sizes[:k]), size) for k, size in enumerate(sizes))
    pieces = len(cuts)
    n1, n2 = (ends, ys) if ends == ys else (ys, ends)
    blocks = n1 * n2
    devices = ends * dps * tps
    dma = lambda n: pltpu.SemaphoreType.DMA((n,))
    one = pltpu.SemaphoreType.DMA
    regular = pltpu.SemaphoreType.REGULAR
    block = lambda n, dtype=BF16: pltpu.VMEM((n, rows, width), dtype)
    state = lambda: pltpu.VMEM((rows, width), F32)
    scratch = [
        block(blocks), block(blocks),
        block((n1 - 1) * n2), block((n1 - 1) * n2),
        block(n2 - 1), block(n2 - 1),
        state(), state(), state(), state(),
        pltpu.VMEM((devices, 1, 128), F32),
        dma(blocks * pieces), dma(3), one, dma(blocks * pieces),
        one, dma((n1 - 1) * n2 * pieces), one, dma((n2 - 1) * pieces),
        one, one,
        one, dma((n1 - 1) * pieces), one, dma((n2 - 1) * pieces),
        one, dma((n1 - 1) * (n2 - 1) * pieces),
        one, one,
        regular, regular, regular, regular, regular,
    ]
    block_bytes = rows * width * 2
    staged = rows_tp * width * 2 > 8 << 20
    if staged:
        scratch += [pltpu.VMEM((rows_tp, width), BF16), one]
    limit = block_bytes * (2 * blocks + 2 * (n1 - 1) * n2 + 2 * (n2 - 1) + 8 + staged * ends * dps) + devices * 4096 + (3 << 20)
    stays = pl.BlockSpec(memory_space=pltpu.HBM)
    vmem = pl.BlockSpec(memory_space=pltpu.VMEM)
    vmem_any = pl.BlockSpec(memory_space=pl.ANY)
    results = pl.pallas_call(
        functools.partial(kernel, (ends, ys, tps, rows, width, cuts, staged)),
        out_shape=(
            (pltpu.HBM if staged else pltpu.VMEM)((rows_tp, width), BF16),
            pltpu.VMEM((rows, width), F32),
            pltpu.VMEM((rows, width), F32),
            pltpu.VMEM((rows, width), F32),
        ),
        in_specs=[stays] * 4,
        out_specs=(stays if staged else vmem,) + (vmem,) * 3,
        scratch_shapes=scratch,
        compiler_params=pltpu.CompilerParams(collective_id=0, has_side_effects=True, vmem_limit_bytes=limit),
        name="sum_update_gather",
    )(*(pltpu.with_memory_space_constraint(x, pltpu.HBM) for x in (grad[0, 0], master[0], moment[0], second[0])))
    first = 1 if staged else 0
    here = results[first:]
    out = pl.pallas_call(
        put_out,
        out_shape=tuple(pltpu.HBM(x.shape, x.dtype) for x in here),
        in_specs=[vmem_any] * len(here),
        out_specs=(stays,) * len(here),
        scratch_shapes=[dma(len(here))],
        compiler_params=pltpu.CompilerParams(vmem_limit_bytes=1 << 20),
        name="put_out",
    )(*(pltpu.with_memory_space_constraint(x, pltpu.VMEM) for x in here))
    weights, master_out, moment_out, second_out = tuple(results[:first]) + tuple(out)
    return (weights, master_out[None], moment_out[None], second_out[None])


def solution(mesh):
    rows = P("tp", ("ends", "dp"), None)
    return jax.shard_map(
        functools.partial(per_device, mesh),
        mesh=mesh,
        in_specs=(P("ends", "dp", "tp", None), rows, rows, rows),
        out_specs=(P("tp", None), rows, rows, rows),
        check_vma=False,
    )
```

```python
import functools
import math

import jax
import jax.numpy as jnp
from jax import lax
from jax.experimental import pallas as pl
from jax.experimental.pallas import tpu as pltpu
from jax.sharding import PartitionSpec as P

STEP = 10
MESH = pl.DeviceIdType.MESH
F32 = jnp.float32
BF16 = jnp.bfloat16
EARLY = 4


def remote(src, dst, send, recv, device):
    return pltpu.make_async_remote_copy(
        src_ref=src, dst_ref=dst, send_sem=send, recv_sem=recv, device_id=device, device_id_type=MESH
    )


def kernel(cfg, grad, master, moment, second, w_out, master_out, moment_out, second_out, *scratch):
    ends, ys, tps, rows, width, cuts, early, staged = cfg
    if staged:
        w_hbm, (w_out, w_sem), scratch = w_out, scratch[-2:], scratch[:-2]
    (own, peer, part1, land1, part2, land2, total, states, squares, terms,
     own_sem, st_sem, peer_s, peer_r, s1, s2, recv, ns, nr, q_s, q_r, qp_r, g_s, g_r, h_s, h_r,
     up, down, here_p, here_1, here_2) = scratch
    e, dp, t = lax.axis_index("ends"), lax.axis_index("dp"), lax.axis_index("tp")
    y, c = dp // 2, lax.rem(dp, 2)
    pieces = len(cuts)
    devices = ends * ys * 2 * tps
    square = ends == ys
    n1, n2 = (ends, ys) if square else (ys, ends)
    blocks = n1 * n2
    first = cuts[0][1]

    def place(core, da, db):
        if square:
            ends_first = core == 0
            de, dy = jnp.where(ends_first, da, db), jnp.where(ends_first, db, da)
        else:
            de, dy = db, da
        return lax.rem(e + de, ends), lax.rem(y + dy, ys)

    def member(core, da, db):
        ee, yy = place(core, da, db)
        return (ee * ys + yy) * 2 + core

    def first_row(core, da, db):
        return pl.multiple_of(member(core, da, db) * rows, rows)

    def at(da, db):
        ee, yy = place(c, da, db)
        return {"ends": ee, "dp": yy * 2 + c}

    partner = {"dp": y * 2 + (1 - c)}
    shifts1, shifts2 = range(1, n1), range(1, n2)
    corners = [(da, db) for da in shifts1 for db in shifts2]
    order = corners + [(0, db) for db in shifts2] + [(da, 0) for da in shifts1] + [(0, 0)]
    slot = lambda da, db: da * n2 + db
    part = lambda k: pl.ds(*cuts[k])

    me = (e * (ys * 2) + dp) * tps + t
    barrier = pltpu.get_barrier_semaphore()
    signal = lambda sem, device: pl.semaphore_signal(sem, inc=1, device_id=device, device_id_type=MESH)
    planes = [at(da, 0) for da in shifts1], [at(0, db) for db in shifts2]
    above, below = {"tp": t + 1}, {"tp": t - 1}
    has_above, has_below = t < tps - 1, t > 0

    for device in planes[0] + planes[1] + [partner]:
        signal(barrier, device)
    pl.when(has_above)(lambda: signal(barrier, above))
    pl.when(has_below)(lambda: signal(barrier, below))

    def rows_at(start, k):
        at_row, size = cuts[k]
        return pl.ds(pl.multiple_of(start + at_row, 16), size)

    def own_copy(da, db):
        i = slot(da, db)
        return pltpu.make_async_copy(grad.at[pl.ds(first_row(c, da, db), rows)], own.at[i], own_sem.at[i])

    for da, db in order:
        own_copy(da, db).start()
    state_copies = [
        pltpu.make_async_copy(src, states.at[i], st_sem.at[i]) for i, src in enumerate((master, moment, second))
    ]
    pl.semaphore_wait(barrier, n1 + n2 - 1 + has_above.astype(jnp.int32) + has_below.astype(jnp.int32))

    def peer_copy(da, db, k):
        i, start = slot(da, db), first_row(1 - c, da, db)
        if da and db:
            sem = peer_r.at[corners.index((da, db)) * pieces + k]
            return remote(grad.at[rows_at(start, k)], peer.at[i, part(k)], peer_s, sem, partner)
        sem = peer_r.at[len(corners) * pieces + order.index((da, db)) - len(corners)]
        return remote(grad.at[pl.ds(start, rows)], peer.at[i], peer_s, sem, partner)

    cut = lambda da, db: pieces if da and db else 1

    for da, db in order:
        for k in range(cut(da, db)):
            peer_copy(da, db, k).start()
    for copy in state_copies:
        copy.start()
    pl.when(jnp.logical_and(has_above, t == 0))(lambda: signal(up, above))
    pl.when(jnp.logical_and(has_below, t == tps - 1))(lambda: signal(down, below))

    def meet(step):
        if step == 0:
            @pl.when(has_below)
            def _():
                pl.semaphore_wait(up, 1)
                pl.when(has_above)(lambda: signal(up, above))
        if step == 1:
            @pl.when(has_above)
            def _():
                pl.semaphore_wait(down, 1)
                pl.when(has_below)(lambda: signal(down, below))
            signal(here_p, partner)
        if step == 2:
            pl.semaphore_wait(here_p, 1)
            for device in planes[0]:
                signal(here_1, device)
        if step == 3:
            pl.semaphore_wait(here_1, n1 - 1)
            for device in planes[1]:
                signal(here_2, device)
        if step == 4:
            pl.semaphore_wait(here_2, n2 - 1)

    def chip_sum(da, db, k):
        i = slot(da, db)
        if k == 0:
            own_copy(da, db).wait()
        if k < cut(da, db):
            peer_copy(da, db, k).wait_recv()
        return own[i, part(k), :].astype(F32) + peer[i, part(k), :].astype(F32)

    def copy1(da, db, k):
        i = (da - 1) * n2 + db
        return remote(part1.at[i, part(k)], land1.at[i, part(k)], s1, recv.at[i * pieces + k], at(da, 0))

    def copy2(db, k):
        i = db - 1
        return remote(part2.at[i, part(k)], land2.at[i, part(k)], s2, recv.at[((n1 - 1) * n2 + i) * pieces + k], at(0, db))

    def send1(da, db, k):
        part1[(da - 1) * n2 + db, part(k), :] = chip_sum(da, db, k).astype(BF16)
        copy1(da, db, k).start()

    def sum1(db, k):
        value = chip_sum(0, db, k)
        for da in shifts1:
            copy1(da, db, k).wait_recv()
            value = value + land1[(da - 1) * n2 + db, part(k), :].astype(F32)
        return value

    for k in range(pieces):
        for da in shifts1:
            for db in shifts2:
                send1(da, db, k)
    for k in range(pieces):
        for da in shifts1:
            send1(da, 0, k)
        for db in shifts2:
            part2[db - 1, part(k), :] = sum1(db, k).astype(BF16)
            copy2(db, k).start()
        if k < 3:
            meet(k)
    for step in range(min(pieces, 3), 4):
        meet(step)
    for copy in state_copies:
        copy.wait()
    mine = member(c, 0, 0)
    for i in range(3):
        terms[mine, i] = states[i, pl.ds(0, first), pl.ds(0, early)].astype(BF16)
    meet(4)
    acc = jnp.zeros((8, width), F32)
    for k in range(pieces):
        value = sum1(0, k)
        for db in shifts2:
            copy2(db, k).wait_recv()
            value = value + land2[db - 1, part(k), :].astype(F32)
        total[part(k), :] = value
        if k == 0:
            terms[mine, 3] = value[:, :early].astype(BF16)
        value = value * value
        for r in range(0, cuts[k][1], 8):
            acc = acc + value[r : r + 8, :]

    lanes = acc[:, :128]
    for j in range(128, width, 128):
        lanes = lanes + acc[:, j : j + 128]
    squares[me] = jnp.sum(lanes, axis=0, keepdims=True)

    high = t >= tps // 2
    for j in range(tps - 1):
        up_from, down_from = j + (t <= j).astype(jnp.int32), tps - 1 - j - (t >= tps - 1 - j).astype(jnp.int32)
        for de in range(ends):
            for ddp in range(ys * 2):
                device = {"ends": lax.rem(e + de, ends), "dp": lax.rem(dp + ddp, ys * 2), "tp": jnp.where(high, up_from, down_from)}
                remote(squares.at[me], squares.at[me], ns, nr, device).start()
    for de in range(ends):
        for ddp in range(ys * 2):
            if de or ddp:
                device = {"ends": lax.rem(e + de, ends), "dp": lax.rem(dp + ddp, ys * 2)}
                remote(squares.at[me], squares.at[me], ns, nr, device).start()

    class Gather:
        def __init__(self, src, count, send, sems, send_p, recv_p):
            self.src, self.count, self.sems, self.send, self.send_p, self.recv_p = src, count, sems, send, send_p, recv_p

        def copy(self, i, da, db, k, device):
            ref = self.src(da, db, k)
            return remote(ref, ref, self.send(k), self.sems.at[i * self.count + k], device)

        def a(self, da, from_da, k):
            return self.copy(da - 1, from_da, 0, k, at(da, 0))

        def b(self, db, from_db, k):
            return self.copy(n1 - 2 + db, 0, from_db, k, at(0, db))

        def f(self, da, db, from_da, from_db, k):
            return self.copy(n1 + n2 - 2 + (da - 1) * (n2 - 1) + db - 1, from_da, from_db, k, at(0, db))

        def p(self, da, db, k):
            ref = self.src(da, db, k)
            remote(ref, ref, self.send_p(k), self.recv_p(k), partner).start()

        def own(self, k):
            for da in shifts1:
                self.a(da, 0, k).start()
            for db in shifts2:
                self.b(db, 0, k).start()
            self.p(0, 0, k)

        def forward(self, k):
            for da in shifts1:
                self.a(da, n1 - da, k).wait_recv()
                for db in shifts2:
                    self.f(da, db, n1 - da, 0, k).start()
                self.p(n1 - da, 0, k)
            for db in shifts2:
                self.b(db, n2 - db, k).wait_recv()
                self.p(0, n2 - db, k)

        def last(self, k):
            for da in shifts1:
                for db in shifts2:
                    self.f(da, db, n1 - da, n2 - db, k).wait_recv()
                    self.p(n1 - da, n2 - db, k)

    halves = 2
    quarter = lambda da, db, k: terms.at[member(c, da, db), pl.ds(4 // halves * k, 4 // halves)]
    ahead = Gather(quarter, halves, lambda k: q_s, q_r, lambda k: q_s, lambda k: qp_r)

    def piece_of(da, db, k):
        here = rows_at(first_row(c, da, db), k)
        return w_out.at[here, pl.ds(early, width - early)] if k == 0 else w_out.at[here]

    gather = Gather(piece_of, pieces, lambda k: g_s if k else h_s, recv, lambda k: g_s if k else h_s, lambda k: g_r if k else h_r)

    for k in range(halves):
        ahead.own(k)
    for k in range(halves):
        ahead.forward(k)
    remote(peer, peer, peer_s, peer_r.at[0], partner).wait_send()
    remote(part1, land1, s1, recv.at[0], partner).wait_send()
    remote(part2, land2, s2, recv.at[0], partner).wait_send()

    others = squares.at[pl.ds(0, devices - 1)]
    everyone = remote(others, others, ns, nr, partner)
    everyone.wait_recv()
    norm2 = jnp.full((8, 128), jnp.sum(jnp.sum(squares[...], axis=0)), F32)
    entries = float(tps * ends * ys * 2 * rows * width)
    factor = jnp.minimum(F32(1.0), F32(math.sqrt(entries)) / (jnp.sqrt(norm2) + 1e-06))[:1, :1]

    def adam(w, m, v, s):
        clipped = factor * s
        m = 0.9 * m + 0.1 * clipped
        v = 0.999 * v + 0.001 * clipped * clipped
        update = m / (1.0 - 0.9**STEP) / (jnp.sqrt(v / (1.0 - 0.999**STEP)) + 1e-08)
        return w - 0.01 * (update + 0.1 * w), m, v

    my_row = first_row(c, 0, 0)

    def step(at_row, size, columns, weights):
        here = pl.ds(at_row, size)
        w, m, v = adam(states[0, here, columns], states[1, here, columns], states[2, here, columns], total[here, columns])
        moment_out[here, columns] = m
        second_out[here, columns] = v
        master_out[here, columns] = w
        if weights:
            w_out[pl.ds(pl.multiple_of(my_row + at_row, 16), size), columns] = w.astype(BF16)

    step(0, first, pl.ds(early, width - early), True)
    gather.own(0)
    for k in range(1, pieces):
        @pl.loop(0, cuts[k][1] // 16)
        def _(g):
            step(pl.multiple_of(cuts[k][0] + g * 16, 16), 16, pl.ds(0, width), True)

        gather.own(k)
    step(0, first, pl.ds(0, early), False)

    for k in range(halves):
        ahead.last(k)
    everyone.wait_send()
    for k in range(pieces):
        gather.forward(k)
        if k == min(1, pieces - 1):
            half = terms.at[pl.ds(0, blocks)]
            remote(half, half, q_s, qp_r, partner).wait_recv()

            @pl.loop(0, 2 * blocks)
            def _(i):
                w, _, _ = adam(*(terms[i, j].astype(F32) for j in range(4)))
                w_out[pl.ds(pl.multiple_of(i * rows, rows), first), pl.ds(0, early)] = w.astype(BF16)

    for k in range(pieces):
        gather.last(k)

    def sized(count, first_piece):
        if first_piece:
            return w_out.at[pl.ds(0, count * first), pl.ds(early, width - early)]
        return w_out.at[pl.ds(0, count * (rows - first))]

    sent = terms.at[pl.ds(0, 2 * blocks - 1)]
    remote(sent, sent, q_s, qp_r, partner).wait_send()
    for first_piece, send, land in ((True, h_s, h_r), (False, g_s, g_r)):
        ref = sized(blocks, first_piece)
        remote(ref, ref, send, land, partner).wait_recv()
        ref = sized(2 * blocks - 1, first_piece)
        remote(ref, ref, send, land, partner).wait_send()
    if staged:
        final = pltpu.make_async_copy(w_out, w_hbm, w_sem)
        final.start()
        final.wait()


def put_out(*refs):
    count = len(refs) // 2
    sems = refs[-1]
    copies = [
        pltpu.make_async_copy(src, dst, sems.at[i])
        for i, (src, dst) in enumerate(zip(refs[:count], refs[count : 2 * count]))
    ]
    for copy in copies:
        copy.start()
    for copy in copies:
        copy.wait()


def per_device(mesh, grad, master, moment, second):
    ends, dps, tps = (mesh.shape[name] for name in ("ends", "dp", "tp"))
    ys = dps // 2
    rows_tp, width = grad.shape[2:]
    rows = rows_tp // (ends * dps)
    sizes = [16] + [32] * (rows // 32 - 1) + [16] if rows % 32 == 0 and rows >= 64 else [rows]
    cuts = tuple((sum(sizes[:k]), size) for k, size in enumerate(sizes))
    pieces = len(cuts)
    n1, n2 = (ends, ys) if ends == ys else (ys, ends)
    blocks = n1 * n2
    devices = ends * dps * tps
    dma = lambda n: pltpu.SemaphoreType.DMA((n,))
    one = pltpu.SemaphoreType.DMA
    regular = pltpu.SemaphoreType.REGULAR
    block = lambda n, dtype=BF16: pltpu.VMEM((n, rows, width), dtype)
    state = lambda: pltpu.VMEM((rows, width), F32)
    early = max(128, width // EARLY // 128 * 128)
    scratch = [
        block(blocks), block(blocks),
        block((n1 - 1) * n2), block((n1 - 1) * n2),
        block(n2 - 1), block(n2 - 1),
        state(), pltpu.VMEM((3, rows, width), F32),
        pltpu.VMEM((devices, 1, 128), F32),
        pltpu.VMEM((2 * blocks, 4, sizes[0], early), BF16),
        dma(blocks), dma(3), one, dma((n1 - 1) * (n2 - 1) * (pieces - 1) + blocks),
        one, one, dma((blocks - 1) * pieces),
        one, one, one, dma((blocks - 1) * 2), one, one, one, one, one,
        regular, regular, regular, regular, regular,
    ]
    block_bytes = rows * width * 2
    staged = rows_tp * width * 2 > 8 << 20
    if staged:
        scratch += [pltpu.VMEM((rows_tp, width), BF16), one]
    limit = block_bytes * (2 * blocks + 2 * (n1 - 1) * n2 + 2 * (n2 - 1) + 8 + staged * ends * dps) + devices * 4096 + 2 * blocks * 8 * sizes[0] * early + (3 << 20)
    stays = pl.BlockSpec(memory_space=pltpu.HBM)
    vmem = pl.BlockSpec(memory_space=pltpu.VMEM)
    vmem_any = pl.BlockSpec(memory_space=pl.ANY)
    results = pl.pallas_call(
        functools.partial(kernel, (ends, ys, tps, rows, width, cuts, early, staged)),
        out_shape=(
            (pltpu.HBM if staged else pltpu.VMEM)((rows_tp, width), BF16),
            pltpu.VMEM((rows, width), F32),
            pltpu.VMEM((rows, width), F32),
            pltpu.VMEM((rows, width), F32),
        ),
        in_specs=[stays] * 4,
        out_specs=(stays if staged else vmem,) + (vmem,) * 3,
        scratch_shapes=scratch,
        compiler_params=pltpu.CompilerParams(collective_id=0, has_side_effects=True, vmem_limit_bytes=limit),
        name="sum_update_gather",
    )(*(pltpu.with_memory_space_constraint(x, pltpu.HBM) for x in (grad[0, 0], master[0], moment[0], second[0])))
    first = 1 if staged else 0
    here = results[first:]
    out = pl.pallas_call(
        put_out,
        out_shape=tuple(pltpu.HBM(x.shape, x.dtype) for x in here),
        in_specs=[vmem_any] * len(here),
        out_specs=(stays,) * len(here),
        scratch_shapes=[dma(len(here))],
        compiler_params=pltpu.CompilerParams(vmem_limit_bytes=1 << 20),
        name="put_out",
    )(*(pltpu.with_memory_space_constraint(x, pltpu.VMEM) for x in here))
    weights, master_out, moment_out, second_out = tuple(results[:first]) + tuple(out)
    return (weights, master_out[None], moment_out[None], second_out[None])


def solution(mesh):
    rows = P("tp", ("ends", "dp"), None)
    return jax.shard_map(
        functools.partial(per_device, mesh),
        mesh=mesh,
        in_specs=(P("ends", "dp", "tp", None), rows, rows, rows),
        out_specs=(P("tp", None), rows, rows, rows),
        check_vma=False,
    )
```

```python
import functools
import math

import jax
import jax.numpy as jnp
from jax import lax
from jax.experimental import pallas as pl
from jax.experimental.pallas import tpu as pltpu
from jax.sharding import PartitionSpec as P

STEP = 10
MESH = pl.DeviceIdType.MESH
F32 = jnp.float32
BF16 = jnp.bfloat16
EARLY = 3


def remote(src, dst, send, recv, device):
    return pltpu.make_async_remote_copy(
        src_ref=src, dst_ref=dst, send_sem=send, recv_sem=recv, device_id=device, device_id_type=MESH
    )


def kernel(cfg, grad, master, moment, second, w_out, master_out, moment_out, second_out, *scratch):
    ends, ys, tps, rows, width, cuts, early, raw, staged = cfg
    if staged:
        w_hbm, (w_out, w_sem), scratch = w_out, scratch[-2:], scratch[:-2]
    (lead, extra, lead_sem, raw_r, own, peer, part1, land1, part2, land2, total, states, squares, terms,
     own_sem, st_sem, peer_s, peer_r, s1, s2, recv, ns, nr, q_s, q_r, qp_r, g_s, g_r, h_s, h_r,
     up, down, here_p, here_1, here_2) = scratch
    e, dp, t = lax.axis_index("ends"), lax.axis_index("dp"), lax.axis_index("tp")
    y, c = dp // 2, lax.rem(dp, 2)
    pieces = len(cuts)
    devices = ends * ys * 2 * tps
    square = ends == ys
    n1, n2 = (ends, ys) if square else (ys, ends)
    blocks = n1 * n2
    first = cuts[0][1]

    def place(core, da, db):
        if square:
            ends_first = core == 0
            de, dy = jnp.where(ends_first, da, db), jnp.where(ends_first, db, da)
        else:
            de, dy = db, da
        return lax.rem(e + de, ends), lax.rem(y + dy, ys)

    def member(core, da, db):
        ee, yy = place(core, da, db)
        return (ee * ys + yy) * 2 + core

    def first_row(core, da, db):
        return pl.multiple_of(member(core, da, db) * rows, rows)

    def at(da, db):
        ee, yy = place(c, da, db)
        return {"ends": ee, "dp": yy * 2 + c}

    partner = {"dp": y * 2 + (1 - c)}
    shifts1, shifts2 = range(1, n1), range(1, n2)
    corners = [(da, db) for da in shifts1 for db in shifts2]
    order = corners + [(0, db) for db in shifts2] + [(da, 0) for da in shifts1] + [(0, 0)]
    slot = lambda da, db: da * n2 + db
    part = lambda k: pl.ds(*cuts[k])

    me = (e * (ys * 2) + dp) * tps + t
    barrier = pltpu.get_barrier_semaphore()
    signal = lambda sem, device: pl.semaphore_signal(sem, inc=1, device_id=device, device_id_type=MESH)
    planes = [at(da, 0) for da in shifts1], [at(0, db) for db in shifts2]
    above, below = {"tp": t + 1}, {"tp": t - 1}
    has_above, has_below = t < tps - 1, t > 0

    def across(core, da):
        ee, yy = place(core, da, 0)
        return {"ends": ee, "dp": yy * 2 + (1 - c)}

    for device in planes[0] + [across(c, da) for da in shifts1] + planes[1] + [partner]:
        signal(barrier, device)
    pl.when(has_above)(lambda: signal(barrier, above))
    pl.when(has_below)(lambda: signal(barrier, below))

    def rows_at(start, k):
        at_row, size = cuts[k]
        return pl.ds(pl.multiple_of(start + at_row, 16), size)

    def own_copy(da, db):
        i = slot(da, db)
        return pltpu.make_async_copy(grad.at[pl.ds(first_row(c, da, db), rows)], own.at[i], own_sem.at[i])

    first_raw = (pl.ds(0, first), pl.ds(0, raw))
    leads = [
        pltpu.make_async_copy(grad.at[rows_at(first_row(1 - c, da, db), 0), pl.ds(0, raw)], lead.at[i], lead_sem.at[i])
        for i, (da, db) in enumerate(corners)
    ]
    for copy in leads:
        copy.start()
    for da, db in corners:
        own_copy(da, db).start()
    state_copies = [
        pltpu.make_async_copy(src, states.at[i], st_sem.at[i]) for i, src in enumerate((master, moment, second))
    ]
    for copy in leads + [own_copy(da, db) for da, db in corners]:
        copy.wait()
    pl.semaphore_wait(barrier, 2 * n1 + n2 - 2 + has_above.astype(jnp.int32) + has_below.astype(jnp.int32))

    def peer_copy(da, db, k):
        i, start = slot(da, db), first_row(1 - c, da, db)
        if da and db:
            sem = peer_r.at[corners.index((da, db)) * pieces + k]
            columns = sum_columns(da, db, k)
            return remote(grad.at[rows_at(start, k), columns], peer.at[i, part(k), columns], peer_s, sem, partner)
        sem = peer_r.at[len(corners) * pieces + order.index((da, db)) - len(corners)]
        return remote(grad.at[pl.ds(start, rows)], peer.at[i], peer_s, sem, partner)

    cut = lambda da, db: pieces if da and db else 1

    def sum_columns(da, db, k):
        return pl.ds(raw, width - raw) if da and db and k == 0 else pl.ds(0, width)

    def raw_copies(i, da, db):
        j = (da - 1) * n2 + db
        mine = remote(own.at[slot(da, db), *first_raw], land1.at[j, *first_raw], s1, raw_r.at[2 * i], at(da, 0))
        return mine, remote(lead.at[i], extra.at[i], peer_s, raw_r.at[2 * i + 1], across(1 - c, da))

    for i, (da, db) in enumerate(corners):
        for copy in raw_copies(i, da, db):
            copy.start()

    for da, db in order:
        for k in range(cut(da, db)):
            peer_copy(da, db, k).start()
    for da, db in order[len(corners):]:
        own_copy(da, db).start()
    for copy in state_copies:
        copy.start()
    pl.when(jnp.logical_and(has_above, t == 0))(lambda: signal(up, above))
    pl.when(jnp.logical_and(has_below, t == tps - 1))(lambda: signal(down, below))

    def meet(step):
        if step == 0:
            @pl.when(has_below)
            def _():
                pl.semaphore_wait(up, 1)
                pl.when(has_above)(lambda: signal(up, above))
        if step == 1:
            @pl.when(has_above)
            def _():
                pl.semaphore_wait(down, 1)
                pl.when(has_below)(lambda: signal(down, below))
            signal(here_p, partner)
        if step == 2:
            pl.semaphore_wait(here_p, 1)
            for device in planes[0]:
                signal(here_1, device)
        if step == 3:
            pl.semaphore_wait(here_1, n1 - 1)
            for device in planes[1]:
                signal(here_2, device)
        if step == 4:
            pl.semaphore_wait(here_2, n2 - 1)

    def chip_sum(da, db, k):
        i = slot(da, db)
        if k == 0 and not (da and db):
            own_copy(da, db).wait()
        if k < cut(da, db):
            peer_copy(da, db, k).wait_recv()
        columns = sum_columns(da, db, k)
        return own[i, part(k), columns].astype(F32) + peer[i, part(k), columns].astype(F32)

    def copy1(da, db, k):
        i = (da - 1) * n2 + db
        columns = sum_columns(da, db, k)
        return remote(part1.at[i, part(k), columns], land1.at[i, part(k), columns], s1, recv.at[i * pieces + k], at(da, 0))

    def copy2(db, k):
        i = db - 1
        return remote(part2.at[i, part(k)], land2.at[i, part(k)], s2, recv.at[((n1 - 1) * n2 + i) * pieces + k], at(0, db))

    def send1(da, db, k):
        part1[(da - 1) * n2 + db, part(k), sum_columns(da, db, k)] = chip_sum(da, db, k).astype(BF16)
        copy1(da, db, k).start()

    def sum1(db, k):
        value = chip_sum(0, db, k)
        for da in shifts1:
            copy1(da, db, k).wait_recv()
            if db and k == 0:
                i = corners.index((da, db))
                for copy in raw_copies(i, da, db):
                    copy.wait_recv()
                there = extra[i].astype(F32)
                value = jnp.concatenate([value[:, :raw] + there, value[:, raw:]], axis=1)
            value = value + land1[(da - 1) * n2 + db, part(k), :].astype(F32)
        return value

    for k in range(pieces):
        for da in shifts1:
            for db in shifts2:
                send1(da, db, k)
    for k in range(pieces):
        for da in shifts1:
            send1(da, 0, k)
        for db in shifts2:
            part2[db - 1, part(k), :] = sum1(db, k).astype(BF16)
            copy2(db, k).start()
        if k < 3:
            meet(k)
    for step in range(min(pieces, 3), 4):
        meet(step)
    for copy in state_copies:
        copy.wait()
    mine = member(c, 0, 0)
    for i in range(3):
        terms[mine, i] = states[i, pl.ds(0, first), pl.ds(0, early)].astype(BF16)
    class Gather:
        def __init__(self, src, count, send, sems, send_p, recv_p):
            self.src, self.count, self.sems, self.send, self.send_p, self.recv_p = src, count, sems, send, send_p, recv_p

        def copy(self, i, da, db, k, device):
            ref = self.src(da, db, k)
            return remote(ref, ref, self.send(k), self.sems.at[i * self.count + k], device)

        def a(self, da, from_da, k):
            return self.copy(da - 1, from_da, 0, k, at(da, 0))

        def b(self, db, from_db, k):
            return self.copy(n1 - 2 + db, 0, from_db, k, at(0, db))

        def f(self, da, db, from_da, from_db, k):
            return self.copy(n1 + n2 - 2 + (da - 1) * (n2 - 1) + db - 1, from_da, from_db, k, at(0, db))

        def p(self, da, db, k):
            ref = self.src(da, db, k)
            remote(ref, ref, self.send_p(k), self.recv_p(k), partner).start()

        def own(self, k):
            for da in shifts1:
                self.a(da, 0, k).start()
            for db in shifts2:
                self.b(db, 0, k).start()
            self.p(0, 0, k)

        def forward(self, k):
            for da in shifts1:
                self.a(da, n1 - da, k).wait_recv()
                for db in shifts2:
                    self.f(da, db, n1 - da, 0, k).start()
                self.p(n1 - da, 0, k)
            for db in shifts2:
                self.b(db, n2 - db, k).wait_recv()
                self.p(0, n2 - db, k)

        def last(self, k):
            for da in shifts1:
                for db in shifts2:
                    self.f(da, db, n1 - da, n2 - db, k).wait_recv()
                    self.p(n1 - da, n2 - db, k)

    halves = 2
    quarter = lambda da, db, k: terms.at[member(c, da, db), pl.ds(4 // halves * k, 4 // halves)]
    ahead = Gather(quarter, halves, lambda k: q_s, q_r, lambda k: q_s, lambda k: qp_r)

    def piece_of(da, db, k):
        here = rows_at(first_row(c, da, db), k)
        return w_out.at[here, pl.ds(early, width - early)] if k == 0 else w_out.at[here]

    gather = Gather(piece_of, pieces, lambda k: g_s if k else h_s, recv, lambda k: g_s if k else h_s, lambda k: g_r if k else h_r)

    meet(4)
    acc = jnp.zeros((8, width), F32)
    for k in range(pieces):
        value = sum1(0, k)
        for db in shifts2:
            copy2(db, k).wait_recv()
            value = value + land2[db - 1, part(k), :].astype(F32)
        total[part(k), :] = value
        if k == 0:
            terms[mine, 3] = value[:, :early].astype(BF16)
        value = value * value
        for r in range(0, cuts[k][1], 8):
            acc = acc + value[r : r + 8, :]
        if k == pieces - 2:
            ahead.own(0)

    lanes = acc[:, :128]
    for j in range(128, width, 128):
        lanes = lanes + acc[:, j : j + 128]
    squares[me] = jnp.sum(lanes, axis=0, keepdims=True)

    high = t >= tps // 2
    for j in range(tps - 1):
        up_from, down_from = j + (t <= j).astype(jnp.int32), tps - 1 - j - (t >= tps - 1 - j).astype(jnp.int32)
        for de in range(ends):
            for ddp in range(ys * 2):
                device = {"ends": lax.rem(e + de, ends), "dp": lax.rem(dp + ddp, ys * 2), "tp": jnp.where(high, up_from, down_from)}
                remote(squares.at[me], squares.at[me], ns, nr, device).start()
    for de in range(ends):
        for ddp in range(ys * 2):
            if de or ddp:
                device = {"ends": lax.rem(e + de, ends), "dp": lax.rem(dp + ddp, ys * 2)}
                remote(squares.at[me], squares.at[me], ns, nr, device).start()

    ahead.own(1)
    for k in range(halves):
        ahead.forward(k)
    remote(peer, peer, peer_s, peer_r.at[0], partner).wait_send()
    remote(part1, land1, s1, recv.at[0], partner).wait_send()
    remote(part2, land2, s2, recv.at[0], partner).wait_send()

    others = squares.at[pl.ds(0, devices - 1)]
    everyone = remote(others, others, ns, nr, partner)
    everyone.wait_recv()
    norm2 = jnp.full((8, 128), jnp.sum(jnp.sum(squares[...], axis=0)), F32)
    entries = float(tps * ends * ys * 2 * rows * width)
    factor = jnp.minimum(F32(1.0), F32(math.sqrt(entries)) / (jnp.sqrt(norm2) + 1e-06))[:1, :1]

    def adam(w, m, v, s):
        clipped = factor * s
        m = 0.9 * m + 0.1 * clipped
        v = 0.999 * v + 0.001 * clipped * clipped
        update = m / (1.0 - 0.9**STEP) / (jnp.sqrt(v / (1.0 - 0.999**STEP)) + 1e-08)
        return w - 0.01 * (update + 0.1 * w), m, v

    my_row = first_row(c, 0, 0)

    def step(at_row, size, columns, weights):
        here = pl.ds(at_row, size)
        w, m, v = adam(states[0, here, columns], states[1, here, columns], states[2, here, columns], total[here, columns])
        moment_out[here, columns] = m
        second_out[here, columns] = v
        master_out[here, columns] = w
        if weights:
            w_out[pl.ds(pl.multiple_of(my_row + at_row, 16), size), columns] = w.astype(BF16)

    step(0, first, pl.ds(early, width - early), True)
    gather.own(0)
    for k in range(1, pieces):
        @pl.loop(0, cuts[k][1] // 16)
        def _(g):
            step(pl.multiple_of(cuts[k][0] + g * 16, 16), 16, pl.ds(0, width), True)

        gather.own(k)
    step(0, first, pl.ds(0, early), False)

    for k in range(halves):
        ahead.last(k)
    everyone.wait_send()
    for k in range(pieces):
        gather.forward(k)
        if k == min(1, pieces - 1):
            half = terms.at[pl.ds(0, blocks)]
            remote(half, half, q_s, qp_r, partner).wait_recv()

            @pl.loop(0, 2 * blocks)
            def _(i):
                w, _, _ = adam(*(terms[i, j].astype(F32) for j in range(4)))
                w_out[pl.ds(pl.multiple_of(i * rows, rows), first), pl.ds(0, early)] = w.astype(BF16)

    for k in range(pieces):
        gather.last(k)

    def sized(count, first_piece):
        if first_piece:
            return w_out.at[pl.ds(0, count * first), pl.ds(early, width - early)]
        return w_out.at[pl.ds(0, count * (rows - first))]

    sent = terms.at[pl.ds(0, 2 * blocks - 1)]
    remote(sent, sent, q_s, qp_r, partner).wait_send()
    for first_piece, send, land in ((True, h_s, h_r), (False, g_s, g_r)):
        ref = sized(blocks, first_piece)
        remote(ref, ref, send, land, partner).wait_recv()
        ref = sized(2 * blocks - 1, first_piece)
        remote(ref, ref, send, land, partner).wait_send()
    if staged:
        final = pltpu.make_async_copy(w_out, w_hbm, w_sem)
        final.start()
        final.wait()


def put_out(*refs):
    count = len(refs) // 2
    sems = refs[-1]
    copies = [
        pltpu.make_async_copy(src, dst, sems.at[i])
        for i, (src, dst) in enumerate(zip(refs[:count], refs[count : 2 * count]))
    ]
    for copy in copies:
        copy.start()
    for copy in copies:
        copy.wait()


def per_device(mesh, grad, master, moment, second):
    ends, dps, tps = (mesh.shape[name] for name in ("ends", "dp", "tp"))
    ys = dps // 2
    rows_tp, width = grad.shape[2:]
    rows = rows_tp // (ends * dps)
    sizes = [16] + [32] * (rows // 32 - 1) + [16] if rows % 32 == 0 and rows >= 64 else [rows]
    cuts = tuple((sum(sizes[:k]), size) for k, size in enumerate(sizes))
    pieces = len(cuts)
    n1, n2 = (ends, ys) if ends == ys else (ys, ends)
    blocks = n1 * n2
    devices = ends * dps * tps
    dma = lambda n: pltpu.SemaphoreType.DMA((n,))
    one = pltpu.SemaphoreType.DMA
    regular = pltpu.SemaphoreType.REGULAR
    block = lambda n, dtype=BF16: pltpu.VMEM((n, rows, width), dtype)
    state = lambda: pltpu.VMEM((rows, width), F32)
    early = max(128, width // EARLY // 128 * 128)
    raw = max(128, width * 2 // 3 // 128 * 128)
    corners = (n1 - 1) * (n2 - 1)
    ahead = lambda: pltpu.VMEM((corners, sizes[0], raw), BF16)
    scratch = [
        ahead(), ahead(), dma(corners), dma(2 * corners),
        block(blocks), block(blocks),
        block((n1 - 1) * n2), block((n1 - 1) * n2),
        block(n2 - 1), block(n2 - 1),
        state(), pltpu.VMEM((3, rows, width), F32),
        pltpu.VMEM((devices, 1, 128), F32),
        pltpu.VMEM((2 * blocks, 4, sizes[0], early), BF16),
        dma(blocks), dma(3), one, dma((n1 - 1) * (n2 - 1) * (pieces - 1) + blocks),
        one, one, dma((blocks - 1) * pieces),
        one, one, one, dma((blocks - 1) * 2), one, one, one, one, one,
        regular, regular, regular, regular, regular,
    ]
    block_bytes = rows * width * 2
    staged = rows_tp * width * 2 > 8 << 20
    if staged:
        scratch += [pltpu.VMEM((rows_tp, width), BF16), one]
    limit = block_bytes * (2 * blocks + 2 * (n1 - 1) * n2 + 2 * (n2 - 1) + 8 + staged * ends * dps) + devices * 4096 + 2 * blocks * 8 * sizes[0] * early + 4 * corners * sizes[0] * raw + (3 << 20)
    stays = pl.BlockSpec(memory_space=pltpu.HBM)
    vmem = pl.BlockSpec(memory_space=pltpu.VMEM)
    vmem_any = pl.BlockSpec(memory_space=pl.ANY)
    results = pl.pallas_call(
        functools.partial(kernel, (ends, ys, tps, rows, width, cuts, early, raw, staged)),
        out_shape=(
            (pltpu.HBM if staged else pltpu.VMEM)((rows_tp, width), BF16),
            pltpu.VMEM((rows, width), F32),
            pltpu.VMEM((rows, width), F32),
            pltpu.VMEM((rows, width), F32),
        ),
        in_specs=[stays] * 4,
        out_specs=(stays if staged else vmem,) + (vmem,) * 3,
        scratch_shapes=scratch,
        compiler_params=pltpu.CompilerParams(collective_id=0, has_side_effects=True, vmem_limit_bytes=limit),
        name="sum_update_gather",
    )(*(pltpu.with_memory_space_constraint(x, pltpu.HBM) for x in (grad[0, 0], master[0], moment[0], second[0])))
    first = 1 if staged else 0
    here = results[first:]
    out = pl.pallas_call(
        put_out,
        out_shape=tuple(pltpu.HBM(x.shape, x.dtype) for x in here),
        in_specs=[vmem_any] * len(here),
        out_specs=(stays,) * len(here),
        scratch_shapes=[dma(len(here))],
        compiler_params=pltpu.CompilerParams(vmem_limit_bytes=1 << 20),
        name="put_out",
    )(*(pltpu.with_memory_space_constraint(x, pltpu.VMEM) for x in here))
    weights, master_out, moment_out, second_out = tuple(results[:first]) + tuple(out)
    return (weights, master_out[None], moment_out[None], second_out[None])


def solution(mesh):
    rows = P("tp", ("ends", "dp"), None)
    return jax.shard_map(
        functools.partial(per_device, mesh),
        mesh=mesh,
        in_specs=(P("ends", "dp", "tp", None), rows, rows, rows),
        out_specs=(P("tp", None), rows, rows, rows),
        check_vma=False,
    )
```

```python
import functools
import math

import jax
import jax.numpy as jnp
from jax import lax
from jax.experimental import pallas as pl
from jax.experimental.pallas import tpu as pltpu
from jax.sharding import PartitionSpec as P

STEP = 10
MESH = pl.DeviceIdType.MESH
F32 = jnp.float32
BF16 = jnp.bfloat16
EARLY = 2


def remote(src, dst, send, recv, device):
    return pltpu.make_async_remote_copy(
        src_ref=src, dst_ref=dst, send_sem=send, recv_sem=recv, device_id=device, device_id_type=MESH
    )


def kernel(cfg, grad, master, moment, second, w_out, master_out, moment_out, second_out, *scratch):
    ends, ys, tps, rows, width, cuts, early, raw, staged = cfg
    if staged:
        w_hbm, (w_out, w_sem), scratch = w_out, scratch[-2:], scratch[:-2]
    (lead, extra, lead_sem, own, peer, part1, land1, part2, land2, total, states, squares, terms,
     own_sem, st_sem, peer_s, peer_r, s1, s2, recv, ns, nr, q_s, up, down, here_p, here_1, here_2) = scratch
    e, dp, t = lax.axis_index("ends"), lax.axis_index("dp"), lax.axis_index("tp")
    y, c = dp // 2, lax.rem(dp, 2)
    pieces = len(cuts)
    devices = ends * ys * 2 * tps
    square = ends == ys
    n1, n2 = (ends, ys) if square else (ys, ends)
    blocks = n1 * n2
    first = cuts[0][1]

    def place(core, da, db):
        if square:
            ends_first = core == 0
            de, dy = jnp.where(ends_first, da, db), jnp.where(ends_first, db, da)
        else:
            de, dy = db, da
        return lax.rem(e + de, ends), lax.rem(y + dy, ys)

    def member(core, da, db):
        ee, yy = place(core, da, db)
        return (ee * ys + yy) * 2 + core

    def first_row(core, da, db):
        return pl.multiple_of(member(core, da, db) * rows, rows)

    def at(da, db):
        ee, yy = place(c, da, db)
        return {"ends": ee, "dp": yy * 2 + c}

    partner = {"dp": y * 2 + (1 - c)}
    shifts1, shifts2 = range(1, n1), range(1, n2)
    corners = [(da, db) for da in shifts1 for db in shifts2]
    order = corners + [(0, db) for db in shifts2] + [(da, 0) for da in shifts1] + [(0, 0)]
    slot = lambda da, db: da * n2 + db
    part = lambda k: pl.ds(*cuts[k])

    me = (e * (ys * 2) + dp) * tps + t
    barrier = pltpu.get_barrier_semaphore()
    signal = lambda sem, device: pl.semaphore_signal(sem, inc=1, device_id=device, device_id_type=MESH)
    planes = [at(da, 0) for da in shifts1], [at(0, db) for db in shifts2]
    above, below = {"tp": t + 1}, {"tp": t - 1}
    has_above, has_below = t < tps - 1, t > 0

    def across(core, da):
        ee, yy = place(core, da, 0)
        return {"ends": ee, "dp": yy * 2 + (1 - c)}

    for device in planes[0] + [across(c, da) for da in shifts1] + planes[1] + [partner]:
        signal(barrier, device)
    pl.when(has_above)(lambda: signal(barrier, above))
    pl.when(has_below)(lambda: signal(barrier, below))

    def rows_at(start, k):
        at_row, size = cuts[k]
        return pl.ds(pl.multiple_of(start + at_row, 16), size)

    def own_copy(da, db):
        i = slot(da, db)
        return pltpu.make_async_copy(grad.at[pl.ds(first_row(c, da, db), rows)], own.at[i], own_sem.at[i])

    first_raw = (pl.ds(0, first), pl.ds(0, raw))
    leads = [
        pltpu.make_async_copy(grad.at[rows_at(first_row(core, da, db), 0), pl.ds(0, raw)], lead.at[2 * i + j], lead_sem.at[2 * i + j])
        for i, (da, db) in enumerate(corners)
        for j, core in enumerate((c, 1 - c))
    ]
    for copy in leads:
        copy.start()
    state_copies = [
        pltpu.make_async_copy(src, states.at[i], st_sem) for i, src in enumerate((master, moment, second))
    ]
    for copy in leads:
        copy.wait()
    for da, db in corners:
        own_copy(da, db).start()
    pl.semaphore_wait(barrier, 2 * n1 + n2 - 2 + has_above.astype(jnp.int32) + has_below.astype(jnp.int32))

    def peer_copy(da, db, k):
        i, start = slot(da, db), first_row(1 - c, da, db)
        if da and db:
            sem = peer_r.at[corners.index((da, db)) * pieces + k]
            columns = sum_columns(da, db, k)
            return remote(grad.at[rows_at(start, k), columns], peer.at[i, part(k), columns], peer_s, sem, partner)
        last = peer_r.shape[0] - 1
        sem = peer_r.at[len(corners) * pieces + order.index((da, db)) - len(corners) if da or db else last]
        return remote(grad.at[pl.ds(start, rows)], peer.at[i], peer_s, sem, partner)

    cut = lambda da, db: pieces if da and db else 1

    def sum_columns(da, db, k):
        return pl.ds(raw, width - raw) if da and db and k == 0 else pl.ds(0, width)

    def raw_copies(i, da, db):
        j = (da - 1) * n2 + db
        mine = remote(lead.at[2 * i], land1.at[j, *first_raw], s1, recv.at[(blocks - 1) * pieces + 2 * i], at(da, 0))
        return mine, remote(lead.at[2 * i + 1], extra.at[i], peer_s, recv.at[(blocks - 1) * pieces + 2 * i + 1], across(1 - c, da))

    for i, (da, db) in enumerate(corners):
        for copy in raw_copies(i, da, db):
            copy.start()

    for da, db in order:
        for k in range(cut(da, db)):
            peer_copy(da, db, k).start()
    for da, db in order[len(corners):]:
        own_copy(da, db).start()
    for copy in state_copies:
        copy.start()
    pl.when(jnp.logical_and(has_above, t == 0))(lambda: signal(up, above))
    pl.when(jnp.logical_and(has_below, t == tps - 1))(lambda: signal(down, below))

    def meet(step):
        if step == 0:
            @pl.when(has_below)
            def _():
                pl.semaphore_wait(up, 1)
                pl.when(has_above)(lambda: signal(up, above))
        if step == 1:
            @pl.when(has_above)
            def _():
                pl.semaphore_wait(down, 1)
                pl.when(has_below)(lambda: signal(down, below))
            signal(here_p, partner)
        if step == 2:
            pl.semaphore_wait(here_p, 1)
            for device in planes[0]:
                signal(here_1, device)
        if step == 3:
            pl.semaphore_wait(here_1, n1 - 1)
            for device in planes[1]:
                signal(here_2, device)
        if step == 4:
            pl.semaphore_wait(here_2, n2 - 1)

    def chip_sum(da, db, k):
        i = slot(da, db)
        if k == 0:
            own_copy(da, db).wait()
        if k < cut(da, db):
            peer_copy(da, db, k).wait_recv()
        columns = sum_columns(da, db, k)
        return own[i, part(k), columns].astype(F32) + peer[i, part(k), columns].astype(F32)

    def copy1(da, db, k):
        i = (da - 1) * n2 + db
        columns = sum_columns(da, db, k)
        return remote(part1.at[i, part(k), columns], land1.at[i, part(k), columns], s1, recv.at[i * pieces + k], at(da, 0))

    def copy2(db, k):
        i = db - 1
        return remote(part2.at[i, part(k)], land2.at[i, part(k)], s2, recv.at[((n1 - 1) * n2 + i) * pieces + k], at(0, db))

    def send1(da, db, k):
        part1[(da - 1) * n2 + db, part(k), sum_columns(da, db, k)] = chip_sum(da, db, k).astype(BF16)
        copy1(da, db, k).start()

    def sum1(db, k):
        value = chip_sum(0, db, k)
        for da in shifts1:
            copy1(da, db, k).wait_recv()
            if db and k == 0:
                i = corners.index((da, db))
                for copy in raw_copies(i, da, db):
                    copy.wait_recv()
                there = extra[i].astype(F32)
                value = jnp.concatenate([value[:, :raw] + there, value[:, raw:]], axis=1)
            value = value + land1[(da - 1) * n2 + db, part(k), :].astype(F32)
        return value

    for k in range(pieces):
        for da in shifts1:
            for db in shifts2:
                send1(da, db, k)
    for k in range(pieces):
        for da in shifts1:
            send1(da, 0, k)
        for db in shifts2:
            part2[db - 1, part(k), :] = sum1(db, k).astype(BF16)
            copy2(db, k).start()
        if k < 3:
            meet(k)
    for step in range(min(pieces, 3), 4):
        meet(step)
    remote(states, states, st_sem, st_sem, partner).wait_recv()
    mine = member(c, 0, 0)
    for i in range(3):
        terms[mine, i] = states[i, pl.ds(0, first), pl.ds(0, early)].astype(BF16)
    class Gather:
        def __init__(self, src, count, send, sems, recv_p, to_both=None):
            self.src, self.count, self.sems, self.send, self.recv_p, self.to_both = src, count, sems, send, recv_p, to_both

        def copy(self, i, da, db, k, device):
            ref = self.src(da, db, k)
            return remote(ref, ref, self.send(k), self.sems.at[i * self.count + k], device)

        def a(self, da, from_da, k):
            return self.copy(da - 1, from_da, 0, k, at(da, 0))

        def b(self, db, from_db, k):
            return self.copy(n1 - 2 + db, 0, from_db, k, at(0, db))

        def f(self, da, db, from_da, from_db, k):
            return self.copy(n1 + n2 - 2 + (da - 1) * (n2 - 1) + db - 1, from_da, from_db, k, at(0, db))

        def p(self, da, db, k):
            ref = self.src(da, db, k)
            remote(ref, ref, self.send(k), self.recv_p(k), partner).start()

        def own(self, k):
            for da in shifts1:
                self.a(da, 0, k).start()
            for db in shifts2:
                self.b(db, 0, k).start()
            self.p(0, 0, k)

        def twin(self, db):
            ee, yy = place(c, 0, db)
            return {"ends": ee, "dp": yy * 2 + (1 - c)}

        def forward(self, k):
            for da in shifts1:
                self.a(da, n1 - da, k).wait_recv()
                for db in shifts2:
                    self.f(da, db, n1 - da, 0, k).start()
                    if k == self.to_both:
                        ref = self.src(n1 - da, 0, k)
                        remote(ref, ref, self.send(k), self.recv_p(k), self.twin(db)).start()
                self.p(n1 - da, 0, k)
            for db in shifts2:
                self.b(db, n2 - db, k).wait_recv()
                self.p(0, n2 - db, k)

        def last(self, k):
            for da in shifts1:
                for db in shifts2:
                    self.f(da, db, n1 - da, n2 - db, k).wait_recv()
                    if k != self.to_both:
                        self.p(n1 - da, n2 - db, k)

    halves = 4
    quarter = lambda da, db, k: terms.at[member(c, da, db), pl.ds(4 // halves * k, 4 // halves)]
    qp_r = own_sem.at[blocks - 1]
    ahead = Gather(quarter, halves, lambda k: q_s, peer_r, lambda k: qp_r)

    tail = width // 256 * 128

    def piece_of(da, db, k):
        start = first_row(c, da, db)
        if k == 0:
            return w_out.at[rows_at(start, 0), pl.ds(early, width - early)]
        if k < pieces - 1:
            return w_out.at[rows_at(start, k)]
        return w_out.at[rows_at(start, pieces - 1), pl.ds(0, tail) if k == pieces - 1 else pl.ds(tail, width - tail)]

    group = lambda k: 0 if k == 0 else 1 if k < pieces - 1 else 2
    sends, lands = (s2, s1, peer_s), [own_sem.at[i] for i in range(3)]
    gather = Gather(piece_of, pieces + 1, lambda k: sends[group(k)], recv, lambda k: lands[group(k)], pieces)

    meet(4)
    acc = jnp.zeros((8, width), F32)
    for k in range(pieces):
        value = sum1(0, k)
        for db in shifts2:
            copy2(db, k).wait_recv()
            value = value + land2[db - 1, part(k), :].astype(F32)
        total[part(k), :] = value
        if k == 0:
            terms[mine, 3] = value[:, :early].astype(BF16)
        value = value * value
        for r in range(0, cuts[k][1], 8):
            acc = acc + value[r : r + 8, :]
        if k == pieces - 2:
            @pl.when(t < tps // 2)
            def _():
                for i in range(3):
                    ahead.own(i)

    lanes = acc[:, :128]
    for j in range(128, width, 128):
        lanes = lanes + acc[:, j : j + 128]
    squares[me] = jnp.sum(lanes, axis=0, keepdims=True)

    high = t >= tps // 2
    for j in range(tps - 1):
        up_from, down_from = j + (t <= j).astype(jnp.int32), tps - 1 - j - (t >= tps - 1 - j).astype(jnp.int32)
        for de in range(ends):
            for ddp in range(ys * 2):
                device = {"ends": lax.rem(e + de, ends), "dp": lax.rem(dp + ddp, ys * 2), "tp": jnp.where(high, up_from, down_from)}
                remote(squares.at[me], squares.at[me], ns, nr, device).start()
    for de in range(ends):
        for ddp in range(ys * 2):
            if de or ddp:
                device = {"ends": lax.rem(e + de, ends), "dp": lax.rem(dp + ddp, ys * 2)}
                remote(squares.at[me], squares.at[me], ns, nr, device).start()

    @pl.when(t >= tps // 2)
    def _():
        for i in range(3):
            ahead.own(i)

    for i in range(3, halves):
        ahead.own(i)
    for k in range(halves):
        ahead.forward(k)
    remote(peer, peer, peer_s, peer_r.at[0], partner).wait_send()
    remote(part1, land1, s1, recv.at[0], partner).wait_send()
    remote(part2, land2, s2, recv.at[0], partner).wait_send()

    others = squares.at[pl.ds(0, devices - 1)]
    everyone = remote(others, others, ns, nr, partner)
    everyone.wait_recv()
    norm2 = jnp.full((8, 128), jnp.sum(jnp.sum(squares[...], axis=0)), F32)
    entries = float(tps * ends * ys * 2 * rows * width)
    factor = jnp.minimum(F32(1.0), F32(math.sqrt(entries)) / (jnp.sqrt(norm2) + 1e-06))[:1, :1]

    def adam(w, m, v, s):
        clipped = factor * s
        m = 0.9 * m + 0.1 * clipped
        v = 0.999 * v + 0.001 * clipped * clipped
        update = m / (1.0 - 0.9**STEP) / (jnp.sqrt(v / (1.0 - 0.999**STEP)) + 1e-08)
        return w - 0.01 * (update + 0.1 * w), m, v

    my_row = first_row(c, 0, 0)

    def step(at_row, size, columns, weights):
        here = pl.ds(at_row, size)
        w, m, v = adam(states[0, here, columns], states[1, here, columns], states[2, here, columns], total[here, columns])
        moment_out[here, columns] = m
        second_out[here, columns] = v
        master_out[here, columns] = w
        if weights:
            w_out[pl.ds(pl.multiple_of(my_row + at_row, 16), size), columns] = w.astype(BF16)

    step(0, first, pl.ds(early, width - early), True)
    gather.own(0)
    for k in range(1, pieces):
        @pl.loop(0, cuts[k][1] // 16)
        def _(g):
            step(pl.multiple_of(cuts[k][0] + g * 16, 16), 16, pl.ds(0, width), True)

        gather.own(k)
    gather.own(pieces)
    step(0, first, pl.ds(0, early), False)

    for k in range(halves):
        ahead.last(k)
    everyone.wait_send()
    for k in range(pieces + 1):
        gather.forward(k)
        if k == 1:
            half = terms.at[pl.ds(0, blocks)]
            remote(half, half, q_s, qp_r, partner).wait_recv()

            @pl.loop(0, 2 * blocks)
            def _(i):
                w, _, _ = adam(*(terms[i, j].astype(F32) for j in range(4)))
                w_out[pl.ds(pl.multiple_of(i * rows, rows), first), pl.ds(0, early)] = w.astype(BF16)

    for k in range(pieces + 1):
        gather.last(k)

    def sized(count, k):
        if k == 0:
            return w_out.at[pl.ds(0, count * first), pl.ds(early, width - early)]
        return w_out.at[pl.ds(0, count * (rows - first - cuts[-1][1] if k == 1 else cuts[-1][1]))]

    sent = terms.at[pl.ds(0, 2 * blocks - 1)]
    remote(sent, sent, q_s, qp_r, partner).wait_send()
    for k in (1, 0, 2):
        ref = sized(blocks, k)
        remote(ref, ref, sends[k], lands[k], partner).wait_recv()
        ref = sized(2 * blocks - 1, k)
        remote(ref, ref, sends[k], lands[k], partner).wait_send()
    if staged:
        final = pltpu.make_async_copy(w_out, w_hbm, w_sem)
        final.start()
        final.wait()


def put_out(*refs):
    count = len(refs) // 2
    sems = refs[-1]
    copies = [
        pltpu.make_async_copy(src, dst, sems.at[i])
        for i, (src, dst) in enumerate(zip(refs[:count], refs[count : 2 * count]))
    ]
    for copy in copies:
        copy.start()
    for copy in copies:
        copy.wait()


def per_device(mesh, grad, master, moment, second):
    ends, dps, tps = (mesh.shape[name] for name in ("ends", "dp", "tp"))
    ys = dps // 2
    rows_tp, width = grad.shape[2:]
    rows = rows_tp // (ends * dps)
    sizes = [16] + [32] * (rows // 32 - 1) + [16] if rows % 32 == 0 and rows >= 64 else [rows]
    cuts = tuple((sum(sizes[:k]), size) for k, size in enumerate(sizes))
    pieces = len(cuts)
    n1, n2 = (ends, ys) if ends == ys else (ys, ends)
    blocks = n1 * n2
    devices = ends * dps * tps
    dma = lambda n: pltpu.SemaphoreType.DMA((n,))
    one = pltpu.SemaphoreType.DMA
    regular = pltpu.SemaphoreType.REGULAR
    block = lambda n, dtype=BF16: pltpu.VMEM((n, rows, width), dtype)
    state = lambda: pltpu.VMEM((rows, width), F32)
    early = max(128, width // EARLY // 128 * 128)
    raw = max(128, width * 2 // 3 // 128 * 128)
    corners = (n1 - 1) * (n2 - 1)
    ahead = lambda count: pltpu.VMEM((count, sizes[0], raw), BF16)
    scratch = [
        ahead(2 * corners), ahead(corners), dma(2 * corners),
        block(blocks), block(blocks),
        block((n1 - 1) * n2), block((n1 - 1) * n2),
        block(n2 - 1), block(n2 - 1),
        state(), pltpu.VMEM((3, rows, width), F32),
        pltpu.VMEM((devices, 1, 128), F32),
        pltpu.VMEM((2 * blocks, 4, sizes[0], early), BF16),
        dma(blocks), one, one, dma(max(corners * (pieces - 1) + blocks, (blocks - 1) * 4 + 1)),
        one, one, dma((blocks - 1) * (pieces + 1)),
        one, one, one,
        regular, regular, regular, regular, regular,
    ]
    block_bytes = rows * width * 2
    staged = rows_tp * width * 2 > 8 << 20
    if staged:
        scratch += [pltpu.VMEM((rows_tp, width), BF16), one]
    limit = block_bytes * (2 * blocks + 2 * (n1 - 1) * n2 + 2 * (n2 - 1) + 8 + staged * ends * dps) + devices * 4096 + 2 * blocks * 8 * sizes[0] * early + 6 * corners * sizes[0] * raw + (3 << 20)
    stays = pl.BlockSpec(memory_space=pltpu.HBM)
    vmem = pl.BlockSpec(memory_space=pltpu.VMEM)
    vmem_any = pl.BlockSpec(memory_space=pl.ANY)
    results = pl.pallas_call(
        functools.partial(kernel, (ends, ys, tps, rows, width, cuts, early, raw, staged)),
        out_shape=(
            (pltpu.HBM if staged else pltpu.VMEM)((rows_tp, width), BF16),
            pltpu.VMEM((rows, width), F32),
            pltpu.VMEM((rows, width), F32),
            pltpu.VMEM((rows, width), F32),
        ),
        in_specs=[stays] * 4,
        out_specs=(stays if staged else vmem,) + (vmem,) * 3,
        scratch_shapes=scratch,
        compiler_params=pltpu.CompilerParams(collective_id=0, has_side_effects=True, vmem_limit_bytes=limit),
        name="sum_update_gather",
    )(*(pltpu.with_memory_space_constraint(x, pltpu.HBM) for x in (grad[0, 0], master[0], moment[0], second[0])))
    first = 1 if staged else 0
    here = results[first:]
    out = pl.pallas_call(
        put_out,
        out_shape=tuple(pltpu.HBM(x.shape, x.dtype) for x in here),
        in_specs=[vmem_any] * len(here),
        out_specs=(stays,) * len(here),
        scratch_shapes=[dma(len(here))],
        compiler_params=pltpu.CompilerParams(vmem_limit_bytes=1 << 20),
        name="put_out",
    )(*(pltpu.with_memory_space_constraint(x, pltpu.VMEM) for x in here))
    weights, master_out, moment_out, second_out = tuple(results[:first]) + tuple(out)
    return (weights, master_out[None], moment_out[None], second_out[None])


def solution(mesh):
    rows = P("tp", ("ends", "dp"), None)
    return jax.shard_map(
        functools.partial(per_device, mesh),
        mesh=mesh,
        in_specs=(P("ends", "dp", "tp", None), rows, rows, rows),
        out_specs=(P("tp", None), rows, rows, rows),
        check_vma=False,
    )
```
